128 devices in a mesh: row: 8 (over z, core), col: 16 (over x, y).
Axes of the slice: x: 4, y: 4, z: 4, core: 2. Of those that a mesh axis runs over, the one named last changes fastest.
Arguments:
- charges: bfloat16 [256, 48, 1024], P(('row', 'col')), may hold values from -6 to 6
- near_blocks: bfloat16 [256, 2, 1024, 1024], P(('row', 'col')), may hold values from -0.125 to 0.125
- near_src: int32 [256, 2], P(('row', 'col')), may hold values from 0 to 255, as said below
- far_v: bfloat16 [128, 128, 1, 32, 1024], P(('row', 'col')), may hold values from -0.1875 to 0.1875
- far_u: bfloat16 [128, 128, 1, 32, 1024], P(('row', 'col')), may hold values from -0.125 to 0.125
- far_rank: int32 [128, 128, 1], P(('row', 'col')), may hold values from 0 to 32, as said below
- far_col: int32 [128, 128, 1], P(('row', 'col')), may hold values from 0 to 1
- far_row: int32 [128, 128, 1], P(('row', 'col')), may hold values from 0 to 1
Outputs:
- potential: float32 [256, 48, 1024], P(('row', 'col'))
The draws below stay inside these ranges and needn't reach their ends.
Inputs may be any that keep to these rules, and one draw needn't show every extreme that they name: near_src[i, n] is a cluster of a device with the same row index as cluster i's device, whose col index differs from it by at most one, cyclically over 16. `far_rank`: in every draw some device receives only used slots (rank above 0) from every device.
All inputs are finite; a program needn't handle non-finite values.
Results may differ from the reference program's by a relative error of at most 0.0017.
Values may be sent and summed in bfloat16 or wider, within the bound.
No kernel may reach another device: no remote copies, remote signals or barrier semaphores. Data moves between devices by JAX's collectives and lax.ppermute only.
A program may use at most 128 MiB of HBM per device.

```python
import jax
import jax.numpy as jnp
from jax import lax

M = 1024
R = 32
RHS = 48
NEAR = 2
FAR_IN = 128
CL_DEV = 2
CLUSTERS = 256
CAP = 1
N_ROW = 8
N_COL = 16
DEVICES = 128


def draw_near_src(key, part):
    first, second = jax.random.split(jax.random.fold_in(key, 11))
    cluster = jnp.arange(CLUSTERS, dtype=jnp.int32)[:, None]
    device = cluster // CL_DEV
    row_index = device // N_COL
    col_index = device % N_COL
    offset = jax.random.randint(first, (CLUSTERS, NEAR), -1, 2)
    within = jax.random.randint(second, (CLUSTERS, NEAR), 0, CL_DEV)
    target = (row_index * N_COL + (col_index + offset + N_COL) % N_COL) * CL_DEV + within
    return target.astype(jnp.int32)


def draw_far_rank(key, part):
    first, second, third = jax.random.split(jax.random.fold_in(key, 23), 3)
    shape = (DEVICES, DEVICES, CAP)
    live = jax.random.randint(first, shape, 0, 10) < 7
    chosen = jax.random.randint(third, (), 0, DEVICES)
    filled = jnp.arange(DEVICES, dtype=jnp.int32)[None, :, None] == chosen
    ranks = jax.random.randint(second, shape, R // 4, R + 1)
    return jnp.where(live | filled, ranks, 0).astype(jnp.int32)


def plant(drawn, stream_key, least, high):
    longest = drawn.shape.index(max(drawn.shape))
    spots = []
    for shift in (0, 1):
        where = [jax.random.randint(jax.random.fold_in(stream_key, axis), (), 0, length) for axis, length in enumerate(drawn.shape)]
        where[longest] = (where[longest] + shift) % drawn.shape[longest]
        spots.append(tuple(where))
    return drawn.at[spots[0]].set(least).at[spots[1]].set(high)


def steps_of(own_key, shape, pieces, smallest, high):
    loudness, own = 1.0, jax.random.fold_in(own_key, 6)
    for dim, parts in pieces:
        steps = jnp.exp(jax.random.uniform(jax.random.fold_in(own, dim), (parts,), jnp.float32, smallest / len(pieces), high / len(pieces)))
        loudness = loudness * jnp.repeat(steps, shape[dim] // parts).reshape([-1 if axis == dim else 1 for axis in range(len(shape))])
    return loudness


def centred(key, dims, scale, reach, pieces=(), held_as=jnp.bfloat16):
    entries = jax.random.normal(key, dims, jnp.float32) * scale
    if len(pieces) > 0:
        entries = steps_of(key, dims, pieces, -0.22, 0.18) * entries
    return jnp.clip(entries, min=-reach, max=reach).astype(held_as)


def setup_inputs(seed: int = 0) -> dict:
    key_list = jax.random.split(jax.random.key(seed), 9)
    charges = centred(key_list[0], (CLUSTERS, RHS, M), 1.0, 6.0, ((0, 128),))
    near_blocks = centred(key_list[1], (CLUSTERS, NEAR, M, M), (NEAR * M) ** -0.5, 0.125, ((0, 128),))
    near_src = draw_near_src(jax.random.fold_in(key_list[8], 71), 0)
    far_v = centred(key_list[3], (DEVICES, DEVICES, CAP, R, M), M ** -0.5, 0.1875, ((0, 128),))
    far_u = centred(key_list[4], (DEVICES, DEVICES, CAP, R, M), (R * FAR_IN // 2) ** -0.5, 0.125, ((0, 128),))
    far_rank = draw_far_rank(jax.random.fold_in(key_list[8], 71), 0)
    far_col = plant(jax.random.randint(key_list[6], (DEVICES, DEVICES, CAP), 0, CL_DEV), jax.random.fold_in(key_list[6], 1), 0, CL_DEV - 1).astype(jnp.int32)
    far_row = plant(jax.random.randint(key_list[7], (DEVICES, DEVICES, CAP), 0, CL_DEV), jax.random.fold_in(key_list[7], 1), 0, CL_DEV - 1).astype(jnp.int32)
    return {"charges": charges, "near_blocks": near_blocks, "near_src": near_src, "far_v": far_v, "far_u": far_u, "far_rank": far_rank, "far_col": far_col, "far_row": far_row}


def reference(charges, near_blocks, near_src, far_v, far_u, far_rank, far_col, far_row):
    devices = N_ROW * N_COL
    width = far_v.shape[3]

    def near_one(item):
        blocks, sources = item
        picked = charges[sources].astype(jnp.float32)
        return jnp.einsum("nsa,nab->sb", picked, blocks.astype(jnp.float32))

    near = lax.map(near_one, (near_blocks, near_src))
    grouped = charges.reshape(devices, CL_DEV, charges.shape[1], charges.shape[2])
    columns = jnp.arange(width, dtype=jnp.int32)

    def send_one(item):
        mine, factors, ranks, picks = item
        selected = mine[picks].astype(jnp.float32)
        proj = jnp.einsum("ecsm,ecrm->ecsr", selected, factors.astype(jnp.float32))
        keep = (columns[None, None, :] < ranks[:, :, None]).astype(jnp.float32)
        return (proj * keep[:, :, None, :]).astype(jnp.bfloat16)

    coef = lax.map(send_one, (grouped, far_v, far_rank, far_col))
    coef_t = jnp.swapaxes(coef, 0, 1)
    locals_ = jnp.arange(CL_DEV, dtype=jnp.int32)

    def receive_one(item):
        incoming, factors, rows = item
        onehot = (rows[:, :, None] == locals_[None, None, :]).astype(jnp.float32)
        spread = incoming.astype(jnp.float32)[:, :, None, :, :] * onehot[:, :, :, None, None]
        return jnp.einsum("dclsr,dcrm->lsm", spread, factors.astype(jnp.float32))

    far = lax.map(receive_one, (coef_t, far_u, far_row))
    far = far.reshape(charges.shape)
    return near + far
```

```python
import functools

import jax
import jax.numpy as jnp
from jax import lax
from jax.experimental import pallas as pl
from jax.experimental.pallas import tpu as pltpu
from jax.sharding import PartitionSpec as P

LANES = 128
V_CHUNKS = 8
N_CHUNKS = 8
STAGED = 32
U_CHUNKS = 3


def lane_pick(values, group):
    picked = values[0]
    for index in range(1, len(values)):
        picked = jnp.where(group == index, values[index], picked)
    return picked


def project_kernel(
    rank_hbm, col_hbm, charges_hbm, v_hbm, out_hbm,
    v_ref, out_ref, charges_ref, rank_ref, col_ref, sems, out_sems,
):
    blocks, width, elements = v_ref.shape
    clusters, rhs, _ = charges_ref.shape
    step = blocks // V_CHUNKS
    small = [
        pltpu.make_async_copy(charges_hbm, charges_ref, sems.at[V_CHUNKS]),
        pltpu.make_async_copy(rank_hbm, rank_ref, sems.at[V_CHUNKS + 1]),
        pltpu.make_async_copy(col_hbm, col_ref, sems.at[V_CHUNKS + 2]),
    ]
    for copy in small:
        copy.start()
    copies = []
    for chunk in range(V_CHUNKS):
        rows = pl.ds(chunk * step, step)
        copies.append(pltpu.make_async_copy(v_hbm.at[rows], v_ref.at[rows], sems.at[chunk]))
        copies[-1].start()
    per = LANES // width
    parts = rhs // 16
    lane = lax.broadcasted_iota(jnp.int32, (16, LANES), 1)
    group = lane // width
    column = lane % width
    for copy in small:
        copy.wait()
    stores = []
    x = charges_ref[...].reshape(clusters * rhs, elements)
    for chunk in range(V_CHUNKS):
        copies[chunk].wait()
        v = v_ref[pl.ds(chunk * step, step)].reshape(step * width, elements)
        proj = lax.dot_general(x, v, (((1,), (1,)), ((), ())), preferred_element_type=jnp.float32)
        for quad in range(step // per):
            first = chunk * step + quad * per
            rank = lane_pick([rank_ref[first + k] for k in range(per)], group)
            col = lane_pick([col_ref[first + k] for k in range(per)], group)
            keep = column < rank
            pieces = []
            for part in range(parts):
                at = slice(quad * LANES, (quad + 1) * LANES)
                value = proj[part * 16 : part * 16 + 16, at]
                for c in range(1, clusters):
                    start = c * rhs + part * 16
                    value = jnp.where(col == c, proj[start : start + 16, at], value)
                pieces.append(jnp.where(keep, value, 0.0))
            for k in range(per):
                message = jnp.zeros((16, LANES), jnp.float32)
                for part in range(parts):
                    shift = (part - k) * width % LANES
                    moved = pltpu.roll(pieces[part], shift, 1) if shift else pieces[part]
                    message = jnp.where(group == part, moved, message)
                out_ref[first + k] = message.astype(jnp.bfloat16)
        rows = pl.ds(chunk * step, step)
        stores.append(pltpu.make_async_copy(out_ref.at[rows], out_hbm.at[rows], out_sems.at[chunk]))
        stores[-1].start()
    for store in stores:
        store.wait()


def near_kernel(
    src_hbm, row_hbm, before_ref, mine_hbm, after_ref, b_hbm, u_hbm,
    near_ref, u_ref, lanes_ref,
    b_ref, x_ref, mine_ref, src_ref, row_ref, sems,
):
    clusters, count, elements, _ = b_ref.shape
    rhs = mine_ref.shape[1]
    last = N_CHUNKS + 1
    small = [
        pltpu.make_async_copy(src_hbm, src_ref, sems.at[last]),
        pltpu.make_async_copy(row_hbm, row_ref, sems.at[last + 1]),
        pltpu.make_async_copy(mine_hbm, mine_ref, sems.at[last + 2]),
    ]
    for copy in small:
        copy.start()
    step = elements * count * clusters // N_CHUNKS
    per = elements // step
    copies = []
    for l in range(clusters):
        for n in range(count):
            for piece in range(per):
                at = (l, n, pl.ds(piece * step, step))
                copies.append(pltpu.make_async_copy(b_hbm.at[at], b_ref.at[at], sems.at[len(copies)]))
                copies[-1].start()
    copies.append(pltpu.make_async_copy(u_hbm.at[pl.ds(0, STAGED)], u_ref, sems.at[N_CHUNKS]))
    copies[-1].start()
    for copy in small:
        copy.wait()
    width = u_ref.shape[1]
    per_row = LANES // width
    group = lax.broadcasted_iota(jnp.int32, (1, LANES), 1) // width
    for quad in range(lanes_ref.shape[0]):
        lanes_ref[quad : quad + 1] = lane_pick([row_ref[quad * per_row + k] for k in range(per_row)], group)
    cols = lax.axis_size("col")
    here = lax.axis_index("col")
    for l in range(clusters):
        for n in range(count):
            source = src_ref[l, n]
            away = lax.rem(lax.rem(source // clusters, cols) - here + 1 + cols, cols)
            which = lax.rem(source, clusters)
            value = mine_ref[which]
            value = jnp.where(away == 0, before_ref[which], value)
            value = jnp.where(away == 2, after_ref[which], value)
            x_ref[l, :, n * elements : (n + 1) * elements] = value
    for l in range(clusters):
        total = None
        for n in range(count):
            for piece in range(per):
                copies[(l * count + n) * per + piece].wait()
                start = n * elements + piece * step
                part = jnp.dot(
                    x_ref[l, :, start : start + step],
                    b_ref[l, n, piece * step : (piece + 1) * step, :],
                    preferred_element_type=jnp.float32,
                )
                total = part if total is None else total + part
        near_ref[l] = total
    copies[N_CHUNKS].wait()


def far_kernel(lanes_ref, in_ref, staged_ref, u_hbm, near_ref, out_ref, u_ref, x_ref, sems):
    kept_blocks, width, elements = staged_ref.shape
    blocks = u_ref.shape[0] // U_CHUNKS
    clusters, rhs, _ = near_ref.shape
    copies = []
    for chunk in range(U_CHUNKS):
        at = pl.ds(chunk * blocks, blocks)
        source = u_hbm.at[pl.ds(kept_blocks + chunk * blocks, blocks)]
        copies.append(pltpu.make_async_copy(source, u_ref.at[at], sems.at[chunk]))
        copies[-1].start()
    per = LANES // width
    parts = rhs // 16
    group = lax.broadcasted_iota(jnp.int32, (16, LANES), 1) // width
    spans = [(0, kept_blocks, staged_ref, 0)]
    for chunk in range(U_CHUNKS):
        spans.append((kept_blocks + chunk * blocks, blocks, u_ref, chunk * blocks))
    total = near_ref[...].reshape(clusters * rhs, elements)
    for index, (begin, size, ref, at) in enumerate(spans):
        for quad in range(begin // per, (begin + size) // per):
            first = quad * per
            row = jnp.broadcast_to(lanes_ref[quad : quad + 1], (16, LANES))
            messages = [in_ref[first + k].astype(jnp.float32) for k in range(per)]
            for part in range(parts):
                value = None
                for k in range(per):
                    shift = (k - part) * width % LANES
                    moved = pltpu.roll(messages[k], shift, 1) if shift else messages[k]
                    value = moved if value is None else jnp.where(group == k, moved, value)
                for l in range(clusters):
                    start = l * rhs + part * 16
                    kept = jnp.where(row == l, value, 0.0).astype(jnp.bfloat16)
                    x_ref[start : start + 16, quad * LANES : (quad + 1) * LANES] = kept
        if index:
            copies[index - 1].wait()
        x = x_ref[:, begin * width : (begin + size) * width]
        u = ref[pl.ds(at, size)].reshape(size * width, elements)
        total = total + jnp.dot(x, u, preferred_element_type=jnp.float32)
    out_ref[...] = total.reshape(clusters, rhs, elements)


def local(charges, near_blocks, near_src, far_v, far_u, far_rank, far_col, far_row):
    clusters, rhs, elements = charges.shape
    devices, width = far_v.shape[1], far_v.shape[3]
    count = near_src.shape[1]
    cols = lax.axis_size("col")
    vmem = pl.BlockSpec(memory_space=pltpu.VMEM)
    hbm = pl.BlockSpec(memory_space=pltpu.HBM)

    def stay(x):
        return pltpu.with_memory_space_constraint(x, pltpu.HBM)

    up = [(i, (i + 1) % cols) for i in range(cols)]
    before = lax.ppermute(charges, "col", up)
    after = lax.ppermute(charges, "col", [(j, i) for i, j in up])
    outgoing = pl.pallas_call(
        project_kernel,
        out_shape=jax.ShapeDtypeStruct((devices, 16, LANES), jnp.bfloat16),
        in_specs=[hbm] * 4,
        out_specs=hbm,
        scratch_shapes=[
            pltpu.VMEM((devices, width, elements), jnp.bfloat16),
            pltpu.VMEM((devices, 16, LANES), jnp.bfloat16),
            pltpu.VMEM(charges.shape, jnp.bfloat16),
            pltpu.SMEM((devices,), jnp.int32),
            pltpu.SMEM((devices,), jnp.int32),
            pltpu.SemaphoreType.DMA((V_CHUNKS + 3,)),
            pltpu.SemaphoreType.DMA((V_CHUNKS,)),
        ],
        compiler_params=pltpu.CompilerParams(vmem_limit_bytes=20 << 20),
        name="project",
    )(
        stay(far_rank.reshape(devices)),
        stay(far_col.reshape(devices)),
        stay(charges),
        stay(far_v.reshape(devices, width, elements)),
    )
    incoming = lax.all_to_all(outgoing, ("row", "col"), split_axis=0, concat_axis=0, tiled=True)
    u = stay(far_u.reshape(devices, width, elements))
    near, staged, lanes = pl.pallas_call(
        near_kernel,
        out_shape=(
            pltpu.VMEM(charges.shape, jnp.float32),
            pltpu.VMEM((STAGED, width, elements), jnp.bfloat16),
            pltpu.VMEM((devices * width // LANES, LANES), jnp.int32),
        ),
        in_specs=[hbm, hbm, vmem, hbm, vmem, hbm, hbm],
        out_specs=(vmem, vmem, vmem),
        scratch_shapes=[
            pltpu.VMEM(near_blocks.shape, jnp.bfloat16),
            pltpu.VMEM((clusters, rhs, count * elements), jnp.bfloat16),
            pltpu.VMEM(charges.shape, jnp.bfloat16),
            pltpu.SMEM(near_src.shape, jnp.int32),
            pltpu.SMEM((devices,), jnp.int32),
            pltpu.SemaphoreType.DMA((N_CHUNKS + 4,)),
        ],
        compiler_params=pltpu.CompilerParams(vmem_limit_bytes=24 << 20),
        cost_estimate=pl.CostEstimate(flops=20_000_000_000, bytes_accessed=10 << 20, transcendentals=0),
        name="near",
    )(
        stay(near_src),
        stay(far_row.reshape(devices)),
        before,
        stay(charges),
        after,
        stay(near_blocks),
        u,
    )
    return pl.pallas_call(
        far_kernel,
        out_shape=jax.ShapeDtypeStruct(charges.shape, jnp.float32),
        in_specs=[vmem, vmem, vmem, hbm, vmem],
        out_specs=vmem,
        scratch_shapes=[
            pltpu.VMEM((devices - STAGED, width, elements), jnp.bfloat16),
            pltpu.VMEM((clusters * rhs, devices * width), jnp.bfloat16),
            pltpu.SemaphoreType.DMA((U_CHUNKS,)),
        ],
        compiler_params=pltpu.CompilerParams(vmem_limit_bytes=24 << 20),
        name="far",
    )(lanes, incoming, staged, u, near)


def solution(mesh):
    return jax.shard_map(
        local,
        mesh=mesh,
        in_specs=(
            P(("row", "col"), None, None),
            P(("row", "col"), None, None, None),
            P(("row", "col"), None),
            P(("row", "col"), None, None, None, None),
            P(("row", "col"), None, None, None, None),
            P(("row", "col"), None, None),
            P(("row", "col"), None, None),
            P(("row", "col"), None, None),
        ),
        out_specs=P(("row", "col"), None, None),
        check_vma=False,
    )
```

```python
import functools

import jax
import jax.numpy as jnp
from jax import lax
from jax.experimental import pallas as pl
from jax.experimental.pallas import tpu as pltpu
from jax.sharding import PartitionSpec as P

LANES = 128
V_SIZES = (16, 32, 32, 32, 16)
N_CHUNKS = 8
STAGED = 32
U_SIZES = (40, 40, 16)
HALVES = 2


def lane_pick(values, group):
    picked = values[0]
    for index in range(1, len(values)):
        picked = jnp.where(group == index, values[index], picked)
    return picked


def offsets(sizes):
    return [sum(sizes[:index]) for index in range(len(sizes))]


def project_kernel(
    rank_hbm, col_hbm, charges_hbm, v_hbm, out_hbm,
    v_ref, out_ref, charges_ref, proj_ref, rank_ref, col_ref, sems, out_sems,
):
    width, elements = v_ref.shape[1:]
    clusters, rhs, _ = charges_ref.shape
    count = len(V_SIZES)
    small = [
        pltpu.make_async_copy(charges_hbm, charges_ref, sems.at[count]),
        pltpu.make_async_copy(rank_hbm, rank_ref, sems.at[count + 1]),
        pltpu.make_async_copy(col_hbm, col_ref, sems.at[count + 2]),
    ]
    for copy in small:
        copy.start()
    begins = offsets(V_SIZES)
    copies = []
    for chunk in range(count):
        rows = pl.ds(begins[chunk], V_SIZES[chunk])
        copies.append(pltpu.make_async_copy(v_hbm.at[rows], v_ref.at[rows], sems.at[chunk]))
        copies[-1].start()
    per = LANES // width
    parts = rhs // 16
    lane = lax.broadcasted_iota(jnp.int32, (16, LANES), 1)
    group = lane // width
    column = lane % width
    for copy in small:
        copy.wait()
    x = charges_ref[...].reshape(clusters * rhs, elements)

    def pack(chunk):
        for quad in range(V_SIZES[chunk] // per):
            first = begins[chunk] + quad * per
            rank = lane_pick([rank_ref[first + k] for k in range(per)], group)
            col = lane_pick([col_ref[first + k] for k in range(per)], group)
            keep = column < rank
            pieces = []
            for part in range(parts):
                at = slice(quad * LANES, (quad + 1) * LANES)
                value = proj_ref[chunk % 2, part * 16 : part * 16 + 16, at]
                for c in range(1, clusters):
                    start = c * rhs + part * 16
                    value = jnp.where(col == c, proj_ref[chunk % 2, start : start + 16, at], value)
                pieces.append(jnp.where(keep, value, 0.0))
            for k in range(per):
                message = jnp.zeros((16, LANES), jnp.float32)
                for part in range(parts):
                    shift = (part - k) * width % LANES
                    moved = pltpu.roll(pieces[part], shift, 1) if shift else pieces[part]
                    message = jnp.where(group == part, moved, message)
                out_ref[first + k] = message.astype(jnp.bfloat16)
        rows = pl.ds(begins[chunk], V_SIZES[chunk])
        stores.append(pltpu.make_async_copy(out_ref.at[rows], out_hbm.at[rows], out_sems.at[chunk]))
        stores[-1].start()

    stores = []
    for chunk in range(count):
        copies[chunk].wait()
        size = V_SIZES[chunk]
        v = v_ref[pl.ds(begins[chunk], size)].reshape(size * width, elements)
        proj_ref[chunk % 2, :, : size * width] = lax.dot_general(
            x, v, (((1,), (1,)), ((), ())), preferred_element_type=jnp.float32
        )
        if chunk:
            pack(chunk - 1)
    pack(count - 1)
    for store in stores:
        store.wait()


def near_kernel(
    src_hbm, row_hbm, first_ref, mine_hbm, second_ref, b_hbm, u_hbm,
    near_ref, u_ref, lanes_ref,
    b_ref, x_ref, mine_ref, src_ref, row_ref, sems,
):
    clusters, count, elements, _ = b_ref.shape
    rhs = mine_ref.shape[1]
    last = N_CHUNKS + 1
    small = [
        pltpu.make_async_copy(src_hbm, src_ref, sems.at[last]),
        pltpu.make_async_copy(row_hbm, row_ref, sems.at[last + 1]),
        pltpu.make_async_copy(mine_hbm, mine_ref, sems.at[last + 2]),
    ]
    for copy in small:
        copy.start()
    step = elements * count * clusters // N_CHUNKS
    per = elements // step
    copies = []
    for l in range(clusters):
        for n in range(count):
            for piece in range(per):
                at = (l, n, pl.ds(piece * step, step))
                copies.append(pltpu.make_async_copy(b_hbm.at[at], b_ref.at[at], sems.at[len(copies)]))
                copies[-1].start()
    copies.append(pltpu.make_async_copy(u_hbm.at[pl.ds(0, STAGED)], u_ref, sems.at[N_CHUNKS]))
    copies[-1].start()
    for copy in small:
        copy.wait()
    width = u_ref.shape[1]
    per_row = LANES // width
    group = lax.broadcasted_iota(jnp.int32, (1, LANES), 1) // width
    for quad in range(lanes_ref.shape[0]):
        lanes_ref[quad : quad + 1] = lane_pick([row_ref[quad * per_row + k] for k in range(per_row)], group)
    cols = lax.axis_size("col")
    here = lax.axis_index("col")
    even = lax.rem(here, 2) == 0
    for l in range(clusters):
        for n in range(count):
            source = src_ref[l, n]
            away = lax.rem(lax.rem(source // clusters, cols) - here + 1 + cols, cols)
            which = lax.rem(source, clusters)
            value = mine_ref[which]
            from_first = away == jnp.where(even, 2, 0)
            from_second = away == jnp.where(even, 0, 2)
            value = jnp.where(from_first, first_ref[which], value)
            value = jnp.where(from_second, second_ref[which], value)
            x_ref[l, :, n * elements : (n + 1) * elements] = value
    for l in range(clusters):
        total = None
        for n in range(count):
            for piece in range(per):
                copies[(l * count + n) * per + piece].wait()
                start = n * elements + piece * step
                part = jnp.dot(
                    x_ref[l, :, start : start + step],
                    b_ref[l, n, piece * step : (piece + 1) * step, :],
                    preferred_element_type=jnp.float32,
                )
                total = part if total is None else total + part
        near_ref[l] = total
    copies[N_CHUNKS].wait()


def far_kernel(
    lanes_ref, in_ref, staged_ref, u_hbm, near_ref, out_hbm, u_ref, x_ref, total_ref, sems, out_sems
):
    kept_blocks, width, elements = staged_ref.shape
    clusters, rhs, _ = near_ref.shape
    copies = []
    spans = [(0, kept_blocks, staged_ref, 0)]
    for chunk, at in enumerate(offsets(U_SIZES)):
        size = U_SIZES[chunk]
        source = u_hbm.at[pl.ds(kept_blocks + at, size)]
        copies.append(pltpu.make_async_copy(source, u_ref.at[pl.ds(at, size)], sems.at[chunk]))
        copies[-1].start()
        spans.append((kept_blocks + at, size, u_ref, at))
    per = LANES // width
    parts = rhs // 16
    group = lax.broadcasted_iota(jnp.int32, (16, LANES), 1) // width

    def unpack(begin, size):
        for quad in range(begin // per, (begin + size) // per):
            first = quad * per
            row = jnp.broadcast_to(lanes_ref[quad : quad + 1], (16, LANES))
            messages = [in_ref[first + k].astype(jnp.float32) for k in range(per)]
            for part in range(parts):
                value = None
                for k in range(per):
                    shift = (k - part) * width % LANES
                    moved = pltpu.roll(messages[k], shift, 1) if shift else messages[k]
                    value = moved if value is None else jnp.where(group == k, moved, value)
                for l in range(clusters):
                    start = l * rhs + part * 16
                    kept = jnp.where(row == l, value, 0.0).astype(jnp.bfloat16)
                    x_ref[start : start + 16, quad * LANES : (quad + 1) * LANES] = kept

    unpack(*spans[0][:2])
    stores = []
    for index, (begin, size, ref, at) in enumerate(spans):
        if index:
            copies[index - 1].wait()
        x = x_ref[:, begin * width : (begin + size) * width]
        final = index == len(spans) - 1
        for half in range(HALVES):
            columns = slice(half * (elements // HALVES), (half + 1) * (elements // HALVES))
            u = ref[at : at + size, :, columns].reshape(size * width, elements // HALVES)
            part = jnp.dot(x, u, preferred_element_type=jnp.float32)
            part = part.reshape(clusters, rhs, elements // HALVES)
            base = total_ref[:, :, columns] if index else near_ref[:, :, columns]
            total_ref[:, :, columns] = base + part
            if final:
                where = (pl.ds(0, clusters), pl.ds(0, rhs), pl.ds(columns.start, elements // HALVES))
                stores.append(pltpu.make_async_copy(total_ref.at[where], out_hbm.at[where], out_sems.at[half]))
                stores[-1].start()
        if not final:
            unpack(*spans[index + 1][:2])
    for store in stores:
        store.wait()


def local(charges, near_blocks, near_src, far_v, far_u, far_rank, far_col, far_row):
    clusters, rhs, elements = charges.shape
    devices, width = far_v.shape[1], far_v.shape[3]
    count = near_src.shape[1]
    cols = lax.axis_size("col")
    vmem = pl.BlockSpec(memory_space=pltpu.VMEM)
    hbm = pl.BlockSpec(memory_space=pltpu.HBM)

    def stay(x):
        return pltpu.with_memory_space_constraint(x, pltpu.HBM)

    pairs = [(i, i + 1) for i in range(0, cols, 2)]
    others = [(i, (i + 1) % cols) for i in range(1, cols, 2)]
    first = lax.ppermute(charges, "col", pairs + [(j, i) for i, j in pairs])
    second = lax.ppermute(charges, "col", others + [(j, i) for i, j in others])
    outgoing = pl.pallas_call(
        project_kernel,
        out_shape=jax.ShapeDtypeStruct((devices, 16, LANES), jnp.bfloat16),
        in_specs=[hbm] * 4,
        out_specs=hbm,
        scratch_shapes=[
            pltpu.VMEM((devices, width, elements), jnp.bfloat16),
            pltpu.VMEM((devices, 16, LANES), jnp.bfloat16),
            pltpu.VMEM(charges.shape, jnp.bfloat16),
            pltpu.VMEM((2, clusters * rhs, max(V_SIZES) * width), jnp.float32),
            pltpu.SMEM((devices,), jnp.int32),
            pltpu.SMEM((devices,), jnp.int32),
            pltpu.SemaphoreType.DMA((len(V_SIZES) + 3,)),
            pltpu.SemaphoreType.DMA((len(V_SIZES),)),
        ],
        compiler_params=pltpu.CompilerParams(vmem_limit_bytes=20 << 20),
        name="project",
    )(
        stay(far_rank.reshape(devices)),
        stay(far_col.reshape(devices)),
        stay(charges),
        stay(far_v.reshape(devices, width, elements)),
    )
    incoming = lax.all_to_all(outgoing, ("row", "col"), split_axis=0, concat_axis=0, tiled=True)
    u = stay(far_u.reshape(devices, width, elements))
    near, staged, lanes = pl.pallas_call(
        near_kernel,
        out_shape=(
            pltpu.VMEM(charges.shape, jnp.float32),
            pltpu.VMEM((STAGED, width, elements), jnp.bfloat16),
            pltpu.VMEM((devices * width // LANES, LANES), jnp.int32),
        ),
        in_specs=[hbm, hbm, vmem, hbm, vmem, hbm, hbm],
        out_specs=(vmem, vmem, vmem),
        scratch_shapes=[
            pltpu.VMEM(near_blocks.shape, jnp.bfloat16),
            pltpu.VMEM((clusters, rhs, count * elements), jnp.bfloat16),
            pltpu.VMEM(charges.shape, jnp.bfloat16),
            pltpu.SMEM(near_src.shape, jnp.int32),
            pltpu.SMEM((devices,), jnp.int32),
            pltpu.SemaphoreType.DMA((N_CHUNKS + 4,)),
        ],
        compiler_params=pltpu.CompilerParams(vmem_limit_bytes=24 << 20),
        cost_estimate=pl.CostEstimate(flops=20_000_000_000, bytes_accessed=10 << 20, transcendentals=0),
        name="near",
    )(
        stay(near_src),
        stay(far_row.reshape(devices)),
        first,
        stay(charges),
        second,
        stay(near_blocks),
        u,
    )
    return pl.pallas_call(
        far_kernel,
        out_shape=jax.ShapeDtypeStruct(charges.shape, jnp.float32),
        in_specs=[vmem, vmem, vmem, hbm, vmem],
        out_specs=hbm,
        scratch_shapes=[
            pltpu.VMEM((devices - STAGED, width, elements), jnp.bfloat16),
            pltpu.VMEM((clusters * rhs, devices * width), jnp.bfloat16),
            pltpu.VMEM(charges.shape, jnp.float32),
            pltpu.SemaphoreType.DMA((len(U_SIZES),)),
            pltpu.SemaphoreType.DMA((HALVES,)),
        ],
        compiler_params=pltpu.CompilerParams(vmem_limit_bytes=24 << 20),
        name="far",
    )(lanes, incoming, staged, u, near)


def solution(mesh):
    return jax.shard_map(
        local,
        mesh=mesh,
        in_specs=(
            P(("row", "col"), None, None),
            P(("row", "col"), None, None, None),
            P(("row", "col"), None),
            P(("row", "col"), None, None, None, None),
            P(("row", "col"), None, None, None, None),
            P(("row", "col"), None, None),
            P(("row", "col"), None, None),
            P(("row", "col"), None, None),
        ),
        out_specs=P(("row", "col"), None, None),
        check_vma=False,
    )
```

```python
import functools

import jax
import jax.numpy as jnp
from jax import lax
from jax.experimental import pallas as pl
from jax.experimental.pallas import tpu as pltpu
from jax.sharding import PartitionSpec as P

LANES = 128
V_SIZES = (16, 32, 32, 32, 16)
N_CHUNKS = 8
STAGED = 32
U_SIZES = (40, 40, 16)
HALVES = 2


def lane_pick(values, group):
    picked = values[0]
    for index in range(1, len(values)):
        picked = jnp.where(group == index, values[index], picked)
    return picked


def block_transpose(tile, width):
    per = LANES // width
    rows = tile.shape[0] // per
    across = lax.broadcasted_iota(jnp.int32, tile.shape, 1) // width
    down = lax.broadcasted_iota(jnp.int32, tile.shape, 0) // rows
    away = lax.rem(across - down + per, per)
    result = tile
    for k in range(1, per):
        moved = pltpu.roll(pltpu.roll(tile, width * k, 1), tile.shape[0] - rows * k, 0)
        result = jnp.where(away == k, moved, result)
    return result


def offsets(sizes):
    return [sum(sizes[:index]) for index in range(len(sizes))]


def project_kernel(
    rank_hbm, col_hbm, charges_hbm, v_hbm, out_hbm,
    v_ref, out_ref, charges_ref, proj_ref, rank_ref, col_ref, sems, out_sems,
):
    width, elements = v_ref.shape[1:]
    clusters, rhs, _ = charges_ref.shape
    count = len(V_SIZES)
    small = [
        pltpu.make_async_copy(charges_hbm, charges_ref, sems.at[count]),
        pltpu.make_async_copy(rank_hbm, rank_ref, sems.at[count + 1]),
        pltpu.make_async_copy(col_hbm, col_ref, sems.at[count + 2]),
    ]
    for copy in small:
        copy.start()
    begins = offsets(V_SIZES)
    copies = []
    for chunk in range(count):
        rows = pl.ds(begins[chunk], V_SIZES[chunk])
        copies.append(pltpu.make_async_copy(v_hbm.at[rows], v_ref.at[rows], sems.at[chunk]))
        copies[-1].start()
    per = LANES // width
    parts = rhs // 16
    lane = lax.broadcasted_iota(jnp.int32, (16, LANES), 1)
    group = lane // width
    column = lane % width
    for copy in small:
        copy.wait()
    x = charges_ref[...].reshape(clusters * rhs, elements)

    def pack(chunk):
        for quad in range(V_SIZES[chunk] // per):
            first = begins[chunk] + quad * per
            rank = lane_pick([rank_ref[first + k] for k in range(per)], group)
            col = lane_pick([col_ref[first + k] for k in range(per)], group)
            keep = column < rank
            at = slice(quad * LANES, (quad + 1) * LANES)
            for part in range(parts):
                value = proj_ref[chunk % 2, part * 16 : part * 16 + 16, at]
                for c in range(1, clusters):
                    start = c * rhs + part * 16
                    value = jnp.where(col == c, proj_ref[chunk % 2, start : start + 16, at], value)
                value = jnp.where(keep, value, 0.0).astype(jnp.bfloat16)
                value = block_transpose(value, width)
                for k in range(per):
                    out_ref[first + k, part] = value[k * 16 // per : (k + 1) * 16 // per]
        rows = pl.ds(begins[chunk], V_SIZES[chunk])
        stores.append(pltpu.make_async_copy(out_ref.at[rows], out_hbm.at[rows], out_sems.at[chunk]))
        stores[-1].start()

    stores = []
    for chunk in range(count):
        copies[chunk].wait()
        size = V_SIZES[chunk]
        v = v_ref[pl.ds(begins[chunk], size)].reshape(size * width, elements)
        proj_ref[chunk % 2, :, : size * width] = lax.dot_general(
            x, v, (((1,), (1,)), ((), ())), preferred_element_type=jnp.float32
        )
        if chunk:
            pack(chunk - 1)
    pack(count - 1)
    for store in stores:
        store.wait()


def near_kernel(
    src_hbm, row_hbm, first_ref, mine_hbm, second_ref, b_hbm, u_hbm,
    near_ref, u_ref, lanes_ref,
    b_ref, x_ref, mine_ref, src_ref, row_ref, sems,
):
    clusters, count, elements, _ = b_ref.shape
    rhs = mine_ref.shape[1]
    last = N_CHUNKS + 1
    small = [
        pltpu.make_async_copy(src_hbm, src_ref, sems.at[last]),
        pltpu.make_async_copy(row_hbm, row_ref, sems.at[last + 1]),
        pltpu.make_async_copy(mine_hbm, mine_ref, sems.at[last + 2]),
    ]
    for copy in small:
        copy.start()
    step = elements * count * clusters // N_CHUNKS
    per = elements // step
    copies = []
    for l in range(clusters):
        for n in range(count):
            for piece in range(per):
                at = (l, n, pl.ds(piece * step, step))
                copies.append(pltpu.make_async_copy(b_hbm.at[at], b_ref.at[at], sems.at[len(copies)]))
                copies[-1].start()
    copies.append(pltpu.make_async_copy(u_hbm.at[pl.ds(0, STAGED)], u_ref, sems.at[N_CHUNKS]))
    copies[-1].start()
    for copy in small:
        copy.wait()
    width = u_ref.shape[1]
    per_row = LANES // width
    group = lax.broadcasted_iota(jnp.int32, (1, LANES), 1) // width
    for quad in range(lanes_ref.shape[0]):
        row = lane_pick([row_ref[quad * per_row + k] for k in range(per_row)], group)
        lanes_ref[quad : quad + 1] = row.astype(jnp.float32)
    cols = lax.axis_size("col")
    here = lax.axis_index("col")
    even = lax.rem(here, 2) == 0
    for l in range(clusters):
        for n in range(count):
            source = src_ref[l, n]
            away = lax.rem(lax.rem(source // clusters, cols) - here + 1 + cols, cols)
            which = lax.rem(source, clusters)
            value = mine_ref[which]
            from_first = away == jnp.where(even, 2, 0)
            from_second = away == jnp.where(even, 0, 2)
            value = jnp.where(from_first, first_ref[which], value)
            value = jnp.where(from_second, second_ref[which], value)
            x_ref[l, :, n * elements : (n + 1) * elements] = value
    for l in range(clusters):
        total = None
        for n in range(count):
            for piece in range(per):
                copies[(l * count + n) * per + piece].wait()
                start = n * elements + piece * step
                part = jnp.dot(
                    x_ref[l, :, start : start + step],
                    b_ref[l, n, piece * step : (piece + 1) * step, :],
                    preferred_element_type=jnp.float32,
                )
                total = part if total is None else total + part
        near_ref[l] = total
    copies[N_CHUNKS].wait()


def far_kernel(
    lanes_ref, in_ref, staged_ref, u_hbm, near_ref, out_hbm, u_ref, x_ref, total_ref, sems, out_sems
):
    kept_blocks, width, elements = staged_ref.shape
    clusters, rhs, _ = near_ref.shape
    copies = []
    spans = [(0, kept_blocks, staged_ref, 0)]
    for chunk, at in enumerate(offsets(U_SIZES)):
        size = U_SIZES[chunk]
        source = u_hbm.at[pl.ds(kept_blocks + at, size)]
        copies.append(pltpu.make_async_copy(source, u_ref.at[pl.ds(at, size)], sems.at[chunk]))
        copies[-1].start()
        spans.append((kept_blocks + at, size, u_ref, at))
    per = LANES // width
    parts = rhs // 16

    def unpack(begin, size):
        for quad in range(begin // per, (begin + size) // per):
            first = quad * per
            row = jnp.broadcast_to(lanes_ref[quad : quad + 1], (16, LANES)).astype(jnp.bfloat16)
            for part in range(parts):
                value = jnp.concatenate([in_ref[first + k, part] for k in range(per)], axis=0)
                value = block_transpose(value, width)
                for l in range(clusters):
                    start = l * rhs + part * 16
                    kept = jnp.where(row == l, value, jnp.zeros_like(value))
                    x_ref[start : start + 16, quad * LANES : (quad + 1) * LANES] = kept

    unpack(*spans[0][:2])
    stores = []
    for index, (begin, size, ref, at) in enumerate(spans):
        if index:
            copies[index - 1].wait()
        x = x_ref[:, begin * width : (begin + size) * width]
        final = index == len(spans) - 1
        for half in range(HALVES):
            columns = slice(half * (elements // HALVES), (half + 1) * (elements // HALVES))
            u = ref[at : at + size, :, columns].reshape(size * width, elements // HALVES)
            part = jnp.dot(x, u, preferred_element_type=jnp.float32)
            part = part.reshape(clusters, rhs, elements // HALVES)
            base = total_ref[:, :, columns] if index else near_ref[:, :, columns]
            total_ref[:, :, columns] = base + part
            if final:
                where = (pl.ds(0, clusters), pl.ds(0, rhs), pl.ds(columns.start, elements // HALVES))
                stores.append(pltpu.make_async_copy(total_ref.at[where], out_hbm.at[where], out_sems.at[half]))
                stores[-1].start()
        if not final:
            unpack(*spans[index + 1][:2])
    for store in stores:
        store.wait()


def local(charges, near_blocks, near_src, far_v, far_u, far_rank, far_col, far_row):
    clusters, rhs, elements = charges.shape
    devices, width = far_v.shape[1], far_v.shape[3]
    count = near_src.shape[1]
    per = LANES // width
    message = (devices, rhs // 16, 16 // per, LANES)
    cols = lax.axis_size("col")
    vmem = pl.BlockSpec(memory_space=pltpu.VMEM)
    hbm = pl.BlockSpec(memory_space=pltpu.HBM)

    def stay(x):
        return pltpu.with_memory_space_constraint(x, pltpu.HBM)

    pairs = [(i, i + 1) for i in range(0, cols, 2)]
    others = [(i, (i + 1) % cols) for i in range(1, cols, 2)]
    first = lax.ppermute(charges, "col", pairs + [(j, i) for i, j in pairs])
    second = lax.ppermute(charges, "col", others + [(j, i) for i, j in others])
    outgoing = pl.pallas_call(
        project_kernel,
        out_shape=jax.ShapeDtypeStruct(message, jnp.bfloat16),
        in_specs=[hbm] * 4,
        out_specs=hbm,
        scratch_shapes=[
            pltpu.VMEM((devices, width, elements), jnp.bfloat16),
            pltpu.VMEM(message, jnp.bfloat16),
            pltpu.VMEM(charges.shape, jnp.bfloat16),
            pltpu.VMEM((2, clusters * rhs, max(V_SIZES) * width), jnp.float32),
            pltpu.SMEM((devices,), jnp.int32),
            pltpu.SMEM((devices,), jnp.int32),
            pltpu.SemaphoreType.DMA((len(V_SIZES) + 3,)),
            pltpu.SemaphoreType.DMA((len(V_SIZES),)),
        ],
        compiler_params=pltpu.CompilerParams(vmem_limit_bytes=20 << 20),
        name="project",
    )(
        stay(far_rank.reshape(devices)),
        stay(far_col.reshape(devices)),
        stay(charges),
        stay(far_v.reshape(devices, width, elements)),
    )
    incoming = lax.all_to_all(outgoing, ("row", "col"), split_axis=0, concat_axis=0, tiled=True)
    u = stay(far_u.reshape(devices, width, elements))
    near, staged, lanes = pl.pallas_call(
        near_kernel,
        out_shape=(
            pltpu.VMEM(charges.shape, jnp.float32),
            pltpu.VMEM((STAGED, width, elements), jnp.bfloat16),
            pltpu.VMEM((devices * width // LANES, LANES), jnp.float32),
        ),
        in_specs=[hbm, hbm, vmem, hbm, vmem, hbm, hbm],
        out_specs=(vmem, vmem, vmem),
        scratch_shapes=[
            pltpu.VMEM(near_blocks.shape, jnp.bfloat16),
            pltpu.VMEM((clusters, rhs, count * elements), jnp.bfloat16),
            pltpu.VMEM(charges.shape, jnp.bfloat16),
            pltpu.SMEM(near_src.shape, jnp.int32),
            pltpu.SMEM((devices,), jnp.int32),
            pltpu.SemaphoreType.DMA((N_CHUNKS + 4,)),
        ],
        compiler_params=pltpu.CompilerParams(vmem_limit_bytes=24 << 20),
        cost_estimate=pl.CostEstimate(flops=20_000_000_000, bytes_accessed=10 << 20, transcendentals=0),
        name="near",
    )(
        stay(near_src),
        stay(far_row.reshape(devices)),
        first,
        stay(charges),
        second,
        stay(near_blocks),
        u,
    )
    return pl.pallas_call(
        far_kernel,
        out_shape=jax.ShapeDtypeStruct(charges.shape, jnp.float32),
        in_specs=[vmem, vmem, vmem, hbm, vmem],
        out_specs=hbm,
        scratch_shapes=[
            pltpu.VMEM((devices - STAGED, width, elements), jnp.bfloat16),
            pltpu.VMEM((clusters * rhs, devices * width), jnp.bfloat16),
            pltpu.VMEM(charges.shape, jnp.float32),
            pltpu.SemaphoreType.DMA((len(U_SIZES),)),
            pltpu.SemaphoreType.DMA((HALVES,)),
        ],
        compiler_params=pltpu.CompilerParams(vmem_limit_bytes=24 << 20),
        name="far",
    )(lanes, incoming, staged, u, near)


def solution(mesh):
    return jax.shard_map(
        local,
        mesh=mesh,
        in_specs=(
            P(("row", "col"), None, None),
            P(("row", "col"), None, None, None),
            P(("row", "col"), None),
            P(("row", "col"), None, None, None, None),
            P(("row", "col"), None, None, None, None),
            P(("row", "col"), None, None),
            P(("row", "col"), None, None),
            P(("row", "col"), None, None),
        ),
        out_specs=P(("row", "col"), None, None),
        check_vma=False,
    )
```

```python
import functools

import jax
import jax.numpy as jnp
from jax import lax
from jax.experimental import pallas as pl
from jax.experimental.pallas import tpu as pltpu
from jax.sharding import PartitionSpec as P

LANES = 128
V_SIZES = (16, 32, 32, 32, 16)
N_CHUNKS = 8
STAGED = 40
U_SIZES = (16, 16, 16, 16, 16, 8)
HALVES = 1


def lane_pick(values, group):
    picked = values[0]
    for index in range(1, len(values)):
        picked = jnp.where(group == index, values[index], picked)
    return picked


def block_transpose(tile, width):
    per = LANES // width
    rows = tile.shape[0] // per
    across = lax.broadcasted_iota(jnp.int32, tile.shape, 1) // width
    down = lax.broadcasted_iota(jnp.int32, tile.shape, 0) // rows
    away = lax.rem(across - down + per, per)
    result = tile
    for k in range(1, per):
        moved = pltpu.roll(pltpu.roll(tile, width * k, 1), tile.shape[0] - rows * k, 0)
        result = jnp.where(away == k, moved, result)
    return result


def offsets(sizes):
    return [sum(sizes[:index]) for index in range(len(sizes))]


def project_kernel(
    rank_hbm, col_hbm, charges_hbm, v_hbm, out_hbm,
    v_ref, out_ref, charges_ref, proj_ref, rank_ref, col_ref, sems, out_sems,
):
    width, elements = v_ref.shape[1:]
    clusters, rhs, _ = charges_ref.shape
    count = len(V_SIZES)
    small = [
        pltpu.make_async_copy(charges_hbm, charges_ref, sems.at[count]),
        pltpu.make_async_copy(rank_hbm, rank_ref, sems.at[count + 1]),
        pltpu.make_async_copy(col_hbm, col_ref, sems.at[count + 2]),
    ]
    for copy in small:
        copy.start()
    begins = offsets(V_SIZES)
    copies = []
    for chunk in range(count):
        rows = pl.ds(begins[chunk], V_SIZES[chunk])
        copies.append(pltpu.make_async_copy(v_hbm.at[rows], v_ref.at[rows], sems.at[chunk]))
        copies[-1].start()
    per = LANES // width
    parts = rhs // 16
    lane = lax.broadcasted_iota(jnp.int32, (16, LANES), 1)
    group = lane // width
    column = lane % width
    for copy in small:
        copy.wait()
    x = charges_ref[...].reshape(clusters * rhs, elements)

    def pack(chunk):
        for quad in range(V_SIZES[chunk] // per):
            first = begins[chunk] + quad * per
            rank = lane_pick([rank_ref[first + k] for k in range(per)], group)
            col = lane_pick([col_ref[first + k] for k in range(per)], group)
            keep = column < rank
            at = slice(quad * LANES, (quad + 1) * LANES)
            for part in range(parts):
                value = proj_ref[chunk % 2, part * 16 : part * 16 + 16, at]
                for c in range(1, clusters):
                    start = c * rhs + part * 16
                    value = jnp.where(col == c, proj_ref[chunk % 2, start : start + 16, at], value)
                value = jnp.where(keep, value, 0.0).astype(jnp.bfloat16)
                value = block_transpose(value, width)
                for k in range(per):
                    out_ref[first + k, part] = value[k * 16 // per : (k + 1) * 16 // per]
        rows = pl.ds(begins[chunk], V_SIZES[chunk])
        stores.append(pltpu.make_async_copy(out_ref.at[rows], out_hbm.at[rows], out_sems.at[chunk]))
        stores[-1].start()

    stores = []
    for chunk in range(count):
        copies[chunk].wait()
        size = V_SIZES[chunk]
        v = v_ref[pl.ds(begins[chunk], size)].reshape(size * width, elements)
        proj_ref[chunk % 2, :, : size * width] = lax.dot_general(
            x, v, (((1,), (1,)), ((), ())), preferred_element_type=jnp.float32
        )
        if chunk:
            pack(chunk - 1)
    pack(count - 1)
    for store in stores:
        store.wait()


def near_kernel(
    src_hbm, row_hbm, first_ref, mine_hbm, second_ref, b_hbm, u_hbm,
    near_hbm, u_ref, lanes_ref,
    b_ref, x_ref, near_ref, mine_ref, src_ref, row_ref, sems,
):
    clusters, count, elements, _ = b_ref.shape
    rhs = mine_ref.shape[1]
    last = N_CHUNKS + 1
    small = [
        pltpu.make_async_copy(src_hbm, src_ref, sems.at[last]),
        pltpu.make_async_copy(row_hbm, row_ref, sems.at[last + 1]),
        pltpu.make_async_copy(mine_hbm, mine_ref, sems.at[last + 2]),
    ]
    for copy in small:
        copy.start()
    step = elements * count * clusters // N_CHUNKS
    per = elements // step
    copies = []
    for l in range(clusters):
        for n in range(count):
            for piece in range(per):
                at = (l, n, pl.ds(piece * step, step))
                copies.append(pltpu.make_async_copy(b_hbm.at[at], b_ref.at[at], sems.at[len(copies)]))
                copies[-1].start()
    copies.append(pltpu.make_async_copy(u_hbm.at[pl.ds(0, STAGED)], u_ref, sems.at[N_CHUNKS]))
    copies[-1].start()
    for copy in small:
        copy.wait()
    width = u_ref.shape[1]
    per_row = LANES // width
    group = lax.broadcasted_iota(jnp.int32, (1, LANES), 1) // width
    for quad in range(lanes_ref.shape[0]):
        row = lane_pick([row_ref[quad * per_row + k] for k in range(per_row)], group)
        lanes_ref[quad : quad + 1] = row.astype(jnp.float32)
    cols = lax.axis_size("col")
    here = lax.axis_index("col")
    even = lax.rem(here, 2) == 0
    for l in range(clusters):
        for n in range(count):
            source = src_ref[l, n]
            away = lax.rem(lax.rem(source // clusters, cols) - here + 1 + cols, cols)
            which = lax.rem(source, clusters)
            value = mine_ref[which]
            from_first = away == jnp.where(even, 2, 0)
            from_second = away == jnp.where(even, 0, 2)
            value = jnp.where(from_first, first_ref[which], value)
            value = jnp.where(from_second, second_ref[which], value)
            x_ref[l, :, n * elements : (n + 1) * elements] = value
    stores = []
    for l in range(clusters):
        total = None
        for n in range(count):
            for piece in range(per):
                copies[(l * count + n) * per + piece].wait()
                start = n * elements + piece * step
                part = jnp.dot(
                    x_ref[l, :, start : start + step],
                    b_ref[l, n, piece * step : (piece + 1) * step, :],
                    preferred_element_type=jnp.float32,
                )
                total = part if total is None else total + part
        near_ref[l] = total
        stores.append(pltpu.make_async_copy(near_ref.at[l], near_hbm.at[l], sems.at[last + 3 + l]))
        stores[-1].start()
    copies[N_CHUNKS].wait()
    for store in stores:
        store.wait()


def far_kernel(
    lanes_ref, in_ref, staged_ref, u_hbm, near_hbm, out_hbm, u_ref, x_ref, total_ref, near_ref, sems, out_sems
):
    kept_blocks, width, elements = staged_ref.shape
    clusters, rhs, _ = total_ref.shape
    fetch = pltpu.make_async_copy(near_hbm, near_ref, sems.at[len(U_SIZES)])
    fetch.start()
    copies = []
    spans = [(0, kept_blocks, staged_ref, 0)]
    for chunk, at in enumerate(offsets(U_SIZES)):
        size = U_SIZES[chunk]
        source = u_hbm.at[pl.ds(kept_blocks + at, size)]
        copies.append(pltpu.make_async_copy(source, u_ref.at[pl.ds(at, size)], sems.at[chunk]))
        copies[-1].start()
        spans.append((kept_blocks + at, size, u_ref, at))
    per = LANES // width
    parts = rhs // 16

    def unpack(begin, size):
        for quad in range(begin // per, (begin + size) // per):
            first = quad * per
            row = jnp.broadcast_to(lanes_ref[quad : quad + 1], (16, LANES)).astype(jnp.bfloat16)
            for part in range(parts):
                value = jnp.concatenate([in_ref[first + k, part] for k in range(per)], axis=0)
                value = block_transpose(value, width)
                for l in range(clusters):
                    start = l * rhs + part * 16
                    kept = jnp.where(row == l, value, jnp.zeros_like(value))
                    x_ref[start : start + 16, quad * LANES : (quad + 1) * LANES] = kept

    unpack(*spans[0][:2])
    stores = []
    for index, (begin, size, ref, at) in enumerate(spans):
        if index:
            copies[index - 1].wait()
        if index == 1:
            fetch.wait()
        x = x_ref[:, begin * width : (begin + size) * width]
        final = index == len(spans) - 1
        for half in range(HALVES):
            columns = slice(half * (elements // HALVES), (half + 1) * (elements // HALVES))
            u = ref[at : at + size, :, columns].reshape(size * width, elements // HALVES)
            part = jnp.dot(x, u, preferred_element_type=jnp.float32)
            part = part.reshape(clusters, rhs, elements // HALVES)
            if index:
                part += total_ref[:, :, columns]
            if index == 1:
                part += near_ref[:, :, columns]
            total_ref[:, :, columns] = part
            if final:
                where = (pl.ds(0, clusters), pl.ds(0, rhs), pl.ds(columns.start, elements // HALVES))
                stores.append(pltpu.make_async_copy(total_ref.at[where], out_hbm.at[where], out_sems.at[half]))
                stores[-1].start()
        if not final:
            unpack(*spans[index + 1][:2])
    for store in stores:
        store.wait()


def local(charges, near_blocks, near_src, far_v, far_u, far_rank, far_col, far_row):
    clusters, rhs, elements = charges.shape
    devices, width = far_v.shape[1], far_v.shape[3]
    count = near_src.shape[1]
    per = LANES // width
    message = (devices, rhs // 16, 16 // per, LANES)
    cols = lax.axis_size("col")
    vmem = pl.BlockSpec(memory_space=pltpu.VMEM)
    hbm = pl.BlockSpec(memory_space=pltpu.HBM)

    def stay(x):
        return pltpu.with_memory_space_constraint(x, pltpu.HBM)

    pairs = [(i, i + 1) for i in range(0, cols, 2)]
    others = [(i, (i + 1) % cols) for i in range(1, cols, 2)]
    first = lax.ppermute(charges, "col", pairs + [(j, i) for i, j in pairs])
    second = lax.ppermute(charges, "col", others + [(j, i) for i, j in others])
    outgoing = pl.pallas_call(
        project_kernel,
        out_shape=jax.ShapeDtypeStruct(message, jnp.bfloat16),
        in_specs=[hbm] * 4,
        out_specs=hbm,
        scratch_shapes=[
            pltpu.VMEM((devices, width, elements), jnp.bfloat16),
            pltpu.VMEM(message, jnp.bfloat16),
            pltpu.VMEM(charges.shape, jnp.bfloat16),
            pltpu.VMEM((2, clusters * rhs, max(V_SIZES) * width), jnp.float32),
            pltpu.SMEM((devices,), jnp.int32),
            pltpu.SMEM((devices,), jnp.int32),
            pltpu.SemaphoreType.DMA((len(V_SIZES) + 3,)),
            pltpu.SemaphoreType.DMA((len(V_SIZES),)),
        ],
        compiler_params=pltpu.CompilerParams(vmem_limit_bytes=20 << 20),
        name="project",
    )(
        stay(far_rank.reshape(devices)),
        stay(far_col.reshape(devices)),
        stay(charges),
        stay(far_v.reshape(devices, width, elements)),
    )
    incoming = lax.all_to_all(outgoing, ("row", "col"), split_axis=0, concat_axis=0, tiled=True)
    u = stay(far_u.reshape(devices, width, elements))
    near, staged, lanes = pl.pallas_call(
        near_kernel,
        out_shape=(
            pltpu.HBM(charges.shape, jnp.float32),
            pltpu.VMEM((STAGED, width, elements), jnp.bfloat16),
            pltpu.VMEM((devices * width // LANES, LANES), jnp.float32),
        ),
        in_specs=[hbm, hbm, vmem, hbm, vmem, hbm, hbm],
        out_specs=(hbm, vmem, vmem),
        scratch_shapes=[
            pltpu.VMEM(near_blocks.shape, jnp.bfloat16),
            pltpu.VMEM((clusters, rhs, count * elements), jnp.bfloat16),
            pltpu.VMEM(charges.shape, jnp.float32),
            pltpu.VMEM(charges.shape, jnp.bfloat16),
            pltpu.SMEM(near_src.shape, jnp.int32),
            pltpu.SMEM((devices,), jnp.int32),
            pltpu.SemaphoreType.DMA((N_CHUNKS + 4 + clusters,)),
        ],
        compiler_params=pltpu.CompilerParams(vmem_limit_bytes=24 << 20),
        cost_estimate=pl.CostEstimate(flops=20_000_000_000, bytes_accessed=10 << 20, transcendentals=0),
        name="near",
    )(
        stay(near_src),
        stay(far_row.reshape(devices)),
        first,
        stay(charges),
        second,
        stay(near_blocks),
        u,
    )
    return pl.pallas_call(
        far_kernel,
        out_shape=jax.ShapeDtypeStruct(charges.shape, jnp.float32),
        in_specs=[vmem, vmem, vmem, hbm, hbm],
        out_specs=hbm,
        scratch_shapes=[
            pltpu.VMEM((devices - STAGED, width, elements), jnp.bfloat16),
            pltpu.VMEM((clusters * rhs, devices * width), jnp.bfloat16),
            pltpu.VMEM(charges.shape, jnp.float32),
            pltpu.VMEM(charges.shape, jnp.float32),
            pltpu.SemaphoreType.DMA((len(U_SIZES) + 1,)),
            pltpu.SemaphoreType.DMA((HALVES,)),
        ],
        compiler_params=pltpu.CompilerParams(vmem_limit_bytes=24 << 20),
        name="far",
    )(lanes, incoming, staged, u, stay(near))


def solution(mesh):
    return jax.shard_map(
        local,
        mesh=mesh,
        in_specs=(
            P(("row", "col"), None, None),
            P(("row", "col"), None, None, None),
            P(("row", "col"), None),
            P(("row", "col"), None, None, None, None),
            P(("row", "col"), None, None, None, None),
            P(("row", "col"), None, None),
            P(("row", "col"), None, None),
            P(("row", "col"), None, None),
        ),
        out_specs=P(("row", "col"), None, None),
        check_vma=False,
    )
```

```python
import functools

import jax
import jax.numpy as jnp
from jax import lax
from jax.experimental import pallas as pl
from jax.experimental.pallas import tpu as pltpu
from jax.sharding import PartitionSpec as P

LANES = 128
V_SIZES = (16, 32, 32, 32, 16)
N_CHUNKS = 8
STAGED = 40
U_SIZES = (16, 16, 16, 16, 16, 8)
HALVES = 1


def lane_pick(values, group):
    picked = values[0]
    for index in range(1, len(values)):
        picked = jnp.where(group == index, values[index], picked)
    return picked


def block_transpose(tile, width):
    per = LANES // width
    rows = tile.shape[0] // per
    across = lax.broadcasted_iota(jnp.int32, tile.shape, 1) // width
    down = lax.broadcasted_iota(jnp.int32, tile.shape, 0) // rows
    away = lax.rem(across - down + per, per)
    result = tile
    for k in range(1, per):
        moved = pltpu.roll(pltpu.roll(tile, width * k, 1), tile.shape[0] - rows * k, 0)
        result = jnp.where(away == k, moved, result)
    return result


def offsets(sizes):
    return [sum(sizes[:index]) for index in range(len(sizes))]


def project_kernel(
    rank_hbm, col_hbm, charges_hbm, v_hbm, out_hbm,
    v_ref, out_ref, charges_ref, proj_ref, rank_ref, col_ref, sems, out_sems,
):
    width, elements = v_ref.shape[1:]
    clusters, rhs, _ = charges_ref.shape
    count = len(V_SIZES)
    small = [
        pltpu.make_async_copy(charges_hbm, charges_ref, sems.at[count]),
        pltpu.make_async_copy(rank_hbm, rank_ref, sems.at[count + 1]),
        pltpu.make_async_copy(col_hbm, col_ref, sems.at[count + 2]),
    ]
    for copy in small:
        copy.start()
    begins = offsets(V_SIZES)
    copies = []
    for chunk in range(count):
        rows = pl.ds(begins[chunk], V_SIZES[chunk])
        copies.append(pltpu.make_async_copy(v_hbm.at[rows], v_ref.at[rows], sems.at[chunk]))
        copies[-1].start()
    per = LANES // width
    parts = rhs // 16
    lane = lax.broadcasted_iota(jnp.int32, (16, LANES), 1)
    group = lane // width
    column = lane % width
    for copy in small:
        copy.wait()
    x = charges_ref[...].reshape(clusters * rhs, elements)

    def pack(chunk):
        for quad in range(V_SIZES[chunk] // per):
            first = begins[chunk] + quad * per
            rank = lane_pick([rank_ref[first + k] for k in range(per)], group)
            col = lane_pick([col_ref[first + k] for k in range(per)], group)
            keep = column < rank
            at = slice(quad * LANES, (quad + 1) * LANES)
            for part in range(parts):
                value = proj_ref[chunk % 2, part * 16 : part * 16 + 16, at]
                for c in range(1, clusters):
                    start = c * rhs + part * 16
                    value = jnp.where(col == c, proj_ref[chunk % 2, start : start + 16, at], value)
                value = jnp.where(keep, value, 0.0).astype(jnp.bfloat16)
                value = block_transpose(value, width)
                for k in range(per):
                    out_ref[first + k, part] = value[k * 16 // per : (k + 1) * 16 // per]
        rows = pl.ds(begins[chunk], V_SIZES[chunk])
        stores.append(pltpu.make_async_copy(out_ref.at[rows], out_hbm.at[rows], out_sems.at[chunk]))
        stores[-1].start()

    stores = []
    for chunk in range(count):
        copies[chunk].wait()
        size = V_SIZES[chunk]
        v = v_ref[pl.ds(begins[chunk], size)].reshape(size * width, elements)
        proj_ref[chunk % 2, :, : size * width] = lax.dot_general(
            x, v, (((1,), (1,)), ((), ())), preferred_element_type=jnp.float32
        )
        if chunk:
            pack(chunk - 1)
    pack(count - 1)
    for store in stores:
        store.wait()


def near_kernel(
    src_hbm, row_hbm, first_ref, mine_hbm, second_ref, b_hbm, u_hbm,
    near_hbm, u_ref, lanes_ref,
    b_ref, x_ref, near_ref, mine_ref, src_ref, row_ref, sems,
):
    clusters, count, elements, _ = b_ref.shape
    rhs = mine_ref.shape[1]
    last = N_CHUNKS + 1
    small = [
        pltpu.make_async_copy(src_hbm, src_ref, sems.at[last]),
        pltpu.make_async_copy(row_hbm, row_ref, sems.at[last + 1]),
        pltpu.make_async_copy(mine_hbm, mine_ref, sems.at[last + 2]),
    ]
    for copy in small:
        copy.start()
    step = elements * count * clusters // N_CHUNKS
    per = elements // step
    copies = []
    for l in range(clusters):
        for n in range(count):
            for piece in range(per):
                at = (l, n, pl.ds(piece * step, step))
                copies.append(pltpu.make_async_copy(b_hbm.at[at], b_ref.at[at], sems.at[len(copies)]))
                copies[-1].start()
    copies.append(pltpu.make_async_copy(u_hbm.at[pl.ds(0, STAGED)], u_ref, sems.at[N_CHUNKS]))
    copies[-1].start()
    for copy in small:
        copy.wait()
    width = u_ref.shape[1]
    per_row = LANES // width
    group = lax.broadcasted_iota(jnp.int32, (1, LANES), 1) // width
    for quad in range(lanes_ref.shape[0]):
        row = lane_pick([row_ref[quad * per_row + k] for k in range(per_row)], group)
        lanes_ref[quad : quad + 1] = row.astype(jnp.float32)
    cols = lax.axis_size("col")
    here = lax.axis_index("col")
    even = lax.rem(here, 2) == 0
    for l in range(clusters):
        for n in range(count):
            source = src_ref[l, n]
            away = lax.rem(lax.rem(source // clusters, cols) - here + 1 + cols, cols)
            which = lax.rem(source, clusters)
            value = mine_ref[which]
            from_first = away == jnp.where(even, 2, 0)
            from_second = away == jnp.where(even, 0, 2)
            value = jnp.where(from_first, first_ref[which], value)
            value = jnp.where(from_second, second_ref[which], value)
            x_ref[l, :, n * elements : (n + 1) * elements] = value
    stores = []
    for l in range(clusters):
        total = None
        for n in range(count):
            for piece in range(per):
                copies[(l * count + n) * per + piece].wait()
                start = n * elements + piece * step
                part = jnp.dot(
                    x_ref[l, :, start : start + step],
                    b_ref[l, n, piece * step : (piece + 1) * step, :],
                    preferred_element_type=jnp.float32,
                )
                total = part if total is None else total + part
        near_ref[l] = total
        stores.append(pltpu.make_async_copy(near_ref.at[l], near_hbm.at[l], sems.at[last + 3 + l]))
        stores[-1].start()
    copies[N_CHUNKS].wait()
    for store in stores:
        store.wait()


def far_kernel(
    lanes_ref, in_ref, staged_ref, u_hbm, near_hbm, out_hbm, u_ref, x_ref, total_ref, near_ref, sems, out_sems
):
    kept_blocks, width, elements = staged_ref.shape
    clusters, rhs, _ = total_ref.shape
    copies = []
    spans = [(0, kept_blocks, staged_ref, 0)]
    for chunk, at in enumerate(offsets(U_SIZES)):
        size = U_SIZES[chunk]
        source = u_hbm.at[pl.ds(kept_blocks + at, size)]
        copies.append(pltpu.make_async_copy(source, u_ref.at[pl.ds(at, size)], sems.at[chunk]))
        copies[-1].start()
        spans.append((kept_blocks + at, size, u_ref, at))
    fetch = pltpu.make_async_copy(near_hbm, near_ref, sems.at[len(U_SIZES)])
    fetch.start()
    per = LANES // width
    parts = rhs // 16

    def unpack(begin, size):
        for quad in range(begin // per, (begin + size) // per):
            first = quad * per
            row = jnp.broadcast_to(lanes_ref[quad : quad + 1], (16, LANES)).astype(jnp.bfloat16)
            for part in range(parts):
                value = jnp.concatenate([in_ref[first + k, part] for k in range(per)], axis=0)
                value = block_transpose(value, width)
                for l in range(clusters):
                    start = l * rhs + part * 16
                    kept = jnp.where(row == l, value, jnp.zeros_like(value))
                    x_ref[start : start + 16, quad * LANES : (quad + 1) * LANES] = kept

    unpack(*spans[0][:2])
    stores = []
    for index, (begin, size, ref, at) in enumerate(spans):
        if index:
            copies[index - 1].wait()
        x = x_ref[:, begin * width : (begin + size) * width]
        final = index == len(spans) - 1
        for half in range(HALVES):
            columns = slice(half * (elements // HALVES), (half + 1) * (elements // HALVES))
            u = ref[at : at + size, :, columns].reshape(size * width, elements // HALVES)
            part = jnp.dot(x, u, preferred_element_type=jnp.float32)
            part = part.reshape(clusters, rhs, elements // HALVES)
            if index:
                part += total_ref[:, :, columns]
            if final:
                if half == 0:
                    fetch.wait()
                part += near_ref[:, :, columns]
            total_ref[:, :, columns] = part
            if final:
                where = (pl.ds(0, clusters), pl.ds(0, rhs), pl.ds(columns.start, elements // HALVES))
                stores.append(pltpu.make_async_copy(total_ref.at[where], out_hbm.at[where], out_sems.at[half]))
                stores[-1].start()
        if not final:
            unpack(*spans[index + 1][:2])
    for store in stores:
        store.wait()


def local(charges, near_blocks, near_src, far_v, far_u, far_rank, far_col, far_row):
    clusters, rhs, elements = charges.shape
    devices, width = far_v.shape[1], far_v.shape[3]
    count = near_src.shape[1]
    per = LANES // width
    message = (devices, rhs // 16, 16 // per, LANES)
    cols = lax.axis_size("col")
    vmem = pl.BlockSpec(memory_space=pltpu.VMEM)
    hbm = pl.BlockSpec(memory_space=pltpu.HBM)

    def stay(x):
        return pltpu.with_memory_space_constraint(x, pltpu.HBM)

    pairs = [(i, i + 1) for i in range(0, cols, 2)]
    others = [(i, (i + 1) % cols) for i in range(1, cols, 2)]
    first = lax.ppermute(charges, "col", pairs + [(j, i) for i, j in pairs])
    second = lax.ppermute(charges, "col", others + [(j, i) for i, j in others])
    outgoing = pl.pallas_call(
        project_kernel,
        out_shape=jax.ShapeDtypeStruct(message, jnp.bfloat16),
        in_specs=[hbm] * 4,
        out_specs=hbm,
        scratch_shapes=[
            pltpu.VMEM((devices, width, elements), jnp.bfloat16),
            pltpu.VMEM(message, jnp.bfloat16),
            pltpu.VMEM(charges.shape, jnp.bfloat16),
            pltpu.VMEM((2, clusters * rhs, max(V_SIZES) * width), jnp.float32),
            pltpu.SMEM((devices,), jnp.int32),
            pltpu.SMEM((devices,), jnp.int32),
            pltpu.SemaphoreType.DMA((len(V_SIZES) + 3,)),
            pltpu.SemaphoreType.DMA((len(V_SIZES),)),
        ],
        compiler_params=pltpu.CompilerParams(vmem_limit_bytes=20 << 20),
        name="project",
    )(
        stay(far_rank.reshape(devices)),
        stay(far_col.reshape(devices)),
        stay(charges),
        stay(far_v.reshape(devices, width, elements)),
    )
    incoming = lax.all_to_all(outgoing, ("row", "col"), split_axis=0, concat_axis=0, tiled=True)
    u = stay(far_u.reshape(devices, width, elements))
    near, staged, lanes = pl.pallas_call(
        near_kernel,
        out_shape=(
            pltpu.HBM(charges.shape, jnp.float32),
            pltpu.VMEM((STAGED, width, elements), jnp.bfloat16),
            pltpu.VMEM((devices * width // LANES, LANES), jnp.float32),
        ),
        in_specs=[hbm, hbm, vmem, hbm, vmem, hbm, hbm],
        out_specs=(hbm, vmem, vmem),
        scratch_shapes=[
            pltpu.VMEM(near_blocks.shape, jnp.bfloat16),
            pltpu.VMEM((clusters, rhs, count * elements), jnp.bfloat16),
            pltpu.VMEM(charges.shape, jnp.float32),
            pltpu.VMEM(charges.shape, jnp.bfloat16),
            pltpu.SMEM(near_src.shape, jnp.int32),
            pltpu.SMEM((devices,), jnp.int32),
            pltpu.SemaphoreType.DMA((N_CHUNKS + 4 + clusters,)),
        ],
        compiler_params=pltpu.CompilerParams(vmem_limit_bytes=24 << 20),
        cost_estimate=pl.CostEstimate(flops=20_000_000_000, bytes_accessed=10 << 20, transcendentals=0),
        name="near",
    )(
        stay(near_src),
        stay(far_row.reshape(devices)),
        first,
        stay(charges),
        second,
        stay(near_blocks),
        u,
    )
    return pl.pallas_call(
        far_kernel,
        out_shape=jax.ShapeDtypeStruct(charges.shape, jnp.float32),
        in_specs=[vmem, vmem, vmem, hbm, hbm],
        out_specs=hbm,
        scratch_shapes=[
            pltpu.VMEM((devices - STAGED, width, elements), jnp.bfloat16),
            pltpu.VMEM((clusters * rhs, devices * width), jnp.bfloat16),
            pltpu.VMEM(charges.shape, jnp.float32),
            pltpu.VMEM(charges.shape, jnp.float32),
            pltpu.SemaphoreType.DMA((len(U_SIZES) + 1,)),
            pltpu.SemaphoreType.DMA((HALVES,)),
        ],
        compiler_params=pltpu.CompilerParams(vmem_limit_bytes=24 << 20),
        name="far",
    )(lanes, incoming, staged, u, stay(near))


def solution(mesh):
    return jax.shard_map(
        local,
        mesh=mesh,
        in_specs=(
            P(("row", "col"), None, None),
            P(("row", "col"), None, None, None),
            P(("row", "col"), None),
            P(("row", "col"), None, None, None, None),
            P(("row", "col"), None, None, None, None),
            P(("row", "col"), None, None),
            P(("row", "col"), None, None),
            P(("row", "col"), None, None),
        ),
        out_specs=P(("row", "col"), None, None),
        check_vma=False,
    )
```
